32 devices in a mesh: term: 4 (over y, x), sector: 8 (over z, core).
Axes of the slice: x: 2, y: 2, z: 4, core: 2. Of those that a mesh axis runs over, the one named last changes fastest.
Arguments:
- wavefunction: float32 [8, 512, 512], P('sector'), may hold values from -120 to 120
- precond: float32 [8, 512, 512], P('sector', 'term'), may hold values from 0.05 to 4
- left_ops: float32 [8, 16, 512, 512], P('sector', 'term'), may hold values from -0.5 to 4.5
- right_ops: float32 [8, 16, 512, 512], P('sector', 'term'), may hold values from -1 to 2
- out_sector: int32 [8, 16], P('sector', 'term'), may hold values from 0 to 7, as said below
- live_counts: int32 [8, 4], P('sector', 'term'), may hold values from 1 to 4, as said below
Outputs:
- first_image: float32 [8, 512, 512], P('sector', 'term')
- correction: float32 [8, 512, 512], P('sector', 'term')
- second_image: float32 [8, 512, 512], P('sector', 'term')
The draws below stay inside these ranges and needn't reach their ends.
Inputs may be any that keep to these rules, and one draw needn't show every extreme that they name: Each term moves the charge by at most one sector: out_sector[s, j] differs from s by at most 1. `live_counts`: in every sector some device has all 4 slots live.
All inputs are finite; a program needn't handle non-finite values.
Results may differ from the reference program's by a relative error of at most 0.0003.
Values sent between devices are 32-bit elements; how exact they have to be, the bound alone decides.
A program may use at most 64 MiB of HBM per device.

```python
import jax
import jax.numpy as jnp
from jax import lax

B = 512
CAP = 4
NSEC = 8
N_TERM = 4


def draw_wavefunction(key, part):
    key_values, key_rows, key_columns = jax.random.split(jax.random.fold_in(key, 11), 3)
    row_index = jnp.arange(B, dtype=jnp.float32)
    jitter = jax.random.uniform(key_rows, (B,), jnp.float32)
    row_scale = 10.0 ** ((row_index + jitter) / B)
    column_scale = 10.0 ** jax.random.uniform(key_columns, (B,), jnp.float32)
    sector_scale = 3.0 ** (jnp.arange(NSEC, dtype=jnp.float32) / max(NSEC - 1, 1))
    values = jax.random.truncated_normal(key_values, -4.0, 4.0, (NSEC, B, B), jnp.float32)
    return 0.1 * values * sector_scale[:, None, None] * row_scale[None, :, None] * column_scale[None, None, :]


def draw_out_sector(key, part):
    change = jax.random.randint(jax.random.fold_in(key, 23), (NSEC, N_TERM * CAP), -1, 2)
    sector_ids = jnp.arange(NSEC, dtype=jnp.int32)[:, None]
    target = sector_ids + change
    target = jnp.where(target < 0, sector_ids + 1, target)
    target = jnp.where(target > NSEC - 1, sector_ids - 1, target)
    return target.astype(jnp.int32)


def draw_live_counts(key, part):
    key_busy, key_pick = jax.random.split(jax.random.fold_in(key, 37), 2)
    busy = jax.random.randint(key_busy, (NSEC, N_TERM), 0, 10) < 3
    counts = jnp.where(busy, CAP, 1)
    chosen = jax.random.randint(key_pick, (NSEC,), 0, N_TERM)
    columns = jnp.arange(N_TERM, dtype=jnp.int32)[None, :]
    counts = jnp.where(columns == chosen[:, None], CAP, counts)
    return counts.astype(jnp.int32)


def sector_strengths(key):
    key_order, key_jitter = jax.random.split(jax.random.fold_in(key, 53), 2)
    order = jax.random.permutation(key_order, NSEC).astype(jnp.float32)
    jitter = jax.random.uniform(key_jitter, (NSEC,), jnp.float32)
    return 4.0 ** ((order + jitter) / NSEC)


def diagonal_weights(key, part):
    targets = draw_out_sector(key, part)
    counts = draw_live_counts(key, part)
    slot_ids = jnp.arange(N_TERM * CAP, dtype=jnp.int32) % CAP
    alive = slot_ids[None, :] < jnp.repeat(counts, CAP, axis=1)
    sector_ids = jnp.arange(NSEC, dtype=jnp.int32)[:, None]
    on_diagonal = jnp.logical_and(alive, targets == sector_ids)
    how_many = jnp.sum(on_diagonal.astype(jnp.float32), axis=1)
    strength = sector_strengths(key)
    effective = jnp.where(how_many > 0.5, strength, 0.0)
    per_slot = jnp.where(on_diagonal, (strength / jnp.maximum(how_many, 1.0))[:, None], 0.0)
    return (per_slot.astype(jnp.float32), effective.astype(jnp.float32))


def draw_left_ops(key, part):
    per_slot, effective = diagonal_weights(key, part)
    noise = jax.random.truncated_normal(jax.random.fold_in(key, 61), -4.0, 4.0, (NSEC, N_TERM * CAP, B, B), jnp.float32)
    noise = noise / jnp.sqrt(jnp.float32(B * N_TERM * CAP))
    identity = jnp.eye(B, dtype=jnp.float32)
    return noise + per_slot[:, :, None, None] * identity[None, None, :, :]


def draw_right_ops(key, part):
    noise = jax.random.truncated_normal(jax.random.fold_in(key, 67), -4.0, 4.0, (NSEC, N_TERM * CAP, B, B), jnp.float32)
    noise = noise / jnp.sqrt(jnp.float32(B))
    identity = jnp.eye(B, dtype=jnp.float32)
    return noise + identity[None, None, :, :]


def draw_precond(key, part):
    per_slot, effective = diagonal_weights(key, part)
    spread = jax.random.uniform(jax.random.fold_in(key, 71), (NSEC, B, B), jnp.float32, 0.0, 1.0)
    entries = 0.25 * 8.0 ** spread
    return entries / (effective + 0.5)[:, None, None]


def setup_inputs(seed: int = 0) -> dict:
    arg_keys = jax.random.split(jax.random.key(seed), 7)
    return {
        "wavefunction": draw_wavefunction(jax.random.fold_in(arg_keys[6], 71), 0),
        "precond": draw_precond(jax.random.fold_in(arg_keys[6], 71), 0),
        "left_ops": draw_left_ops(jax.random.fold_in(arg_keys[6], 71), 0),
        "right_ops": draw_right_ops(jax.random.fold_in(arg_keys[6], 71), 0),
        "out_sector": draw_out_sector(jax.random.fold_in(arg_keys[6], 71), 0),
        "live_counts": draw_live_counts(jax.random.fold_in(arg_keys[6], 71), 0),
    }


def matmul(first_op, second_op):
    return jnp.dot(first_op, second_op, precision=lax.Precision.HIGHEST, preferred_element_type=jnp.float32)


def apply_hamiltonian(field, left_ops, right_ops, out_sector, alive):
    def sector_step(totals, inputs):
        center, left_stack, right_stack, destinations, flags = inputs

        def slot_step(running, slot_data):
            left_one, right_one, destination, alive_flag = slot_data
            product = matmul(matmul(left_one, center), right_one)
            return running.at[destination].add(product * alive_flag), None

        totals, _ = lax.scan(slot_step, totals, (left_stack, right_stack, destinations, flags))
        return totals, None

    totals, _ = lax.scan(sector_step, jnp.zeros_like(field), (field, left_ops, right_ops, out_sector, alive))
    return totals


def reference(wavefunction, precond, left_ops, right_ops, out_sector, live_counts):
    slot_ids = jnp.arange(N_TERM * CAP, dtype=jnp.int32) % CAP
    alive = (slot_ids[None, :] < jnp.repeat(live_counts, CAP, axis=1)).astype(jnp.float32)
    first_image = apply_hamiltonian(wavefunction, left_ops, right_ops, out_sector, alive)
    norm_sq = jnp.sum(wavefunction * wavefunction)
    rayleigh = jnp.sum(wavefunction * first_image) / norm_sq
    raw = precond * (first_image - rayleigh * wavefunction)
    correction = raw - (jnp.sum(wavefunction * raw) / norm_sq) * wavefunction
    second_image = apply_hamiltonian(correction, left_ops, right_ops, out_sector, alive)
    return first_image, correction, second_image
```

```python
import functools

import jax
import jax.numpy as jnp
from jax import lax
from jax.experimental import pallas as pl
from jax.experimental.pallas import tpu as pltpu
from jax.sharding import PartitionSpec as P

F32 = jnp.float32
MESH = pl.DeviceIdType.MESH
VMEM = pl.BlockSpec(memory_space=pltpu.VMEM)


def split(x):
    high = x.astype(jnp.bfloat16)
    return high, (x - high.astype(F32)).astype(jnp.bfloat16)


def product(a_high, a_low, b_high, b_low):
    dot = functools.partial(jnp.dot, preferred_element_type=F32)
    return dot(a_high, b_high) + dot(a_high, b_low) + dot(a_low, b_high)


def terms_kernel(target, count, v_ref, left_ref, right_ref, out_ref, v_high, v_low, r_high, r_low):
    slot = pl.program_id(0)
    width = v_ref.shape[0]
    piece = min(256, width)

    @pl.when(slot == 0)
    def _():
        out_ref[...] = jnp.zeros_like(out_ref)
        v_high[...], v_low[...] = split(v_ref[...])

    @pl.when(slot < count[0, 0])
    def _():
        place = target[0, slot] - lax.axis_index("sector") + 1
        r_high[...], r_low[...] = split(right_ref[...])
        for start in range(0, width, piece):
            rows = pl.ds(start, piece)
            left_high, left_low = split(left_ref[rows])
            inner = product(left_high, left_low, v_high[...], v_low[...])
            in_high, in_low = split(inner)
            out_ref[place, rows] += product(in_high, in_low, r_high[...], r_low[...])


def all_terms(vector, left_ops, right_ops, out_sector, live_counts):
    slots, width = left_ops.shape[1], left_ops.shape[2]

    def live(j, target, count):
        return (0, jnp.minimum(j, count[0, 0] - 1), 0, 0)

    return pl.pallas_call(
        terms_kernel,
        out_shape=jax.ShapeDtypeStruct((3, width, width), F32),
        grid_spec=pltpu.PrefetchScalarGridSpec(
            num_scalar_prefetch=2,
            grid=(slots,),
            in_specs=[
                pl.BlockSpec((width, width), lambda j, a, b: (0, 0)),
                pl.BlockSpec((None, None, width, width), live),
                pl.BlockSpec((None, None, width, width), live),
            ],
            out_specs=pl.BlockSpec((3, width, width), lambda j, a, b: (0, 0, 0)),
            scratch_shapes=[pltpu.VMEM((width, width), jnp.bfloat16)] * 4,
        ),
        compiler_params=pltpu.CompilerParams(dimension_semantics=("arbitrary",), vmem_limit_bytes=40 << 20),
    )(out_sector, live_counts, vector, left_ops, right_ops)


def send(source, target, send_sem, recv_sem, **where):
    return pltpu.make_async_remote_copy(
        src_ref=source, dst_ref=target, send_sem=send_sem, recv_sem=recv_sem,
        device_id=where, device_id_type=MESH,
    )


def greet():
    terms, sectors = lax.axis_size("term"), lax.axis_size("sector")
    t, s = lax.axis_index("term"), lax.axis_index("sector")
    barrier = pltpu.get_barrier_semaphore()
    for k in range(1, terms):
        pl.semaphore_signal(barrier, inc=1, device_id={"term": lax.rem(t + k, terms)}, device_id_type=MESH)
    for k in range(1, sectors):
        pl.semaphore_signal(barrier, inc=1, device_id={"sector": lax.rem(s + k, sectors)}, device_id_type=MESH)
    pl.semaphore_wait(barrier, terms + sectors - 2)


def exchange(whole, image, bufs):
    up_in, down_in, acc, rs_in, up_s, up_r, down_s, down_r, rs_s, rs_r = bufs
    terms, sectors = lax.axis_size("term"), lax.axis_size("sector")
    t, s = lax.axis_index("term"), lax.axis_index("sector")
    rows = whole.shape[1] // terms

    def slab(r):
        return pl.ds(pl.multiple_of(r * rows, rows), rows)

    def upward(r):
        return send(whole.at[2, slab(r)], up_in.at[slab(r)], up_s.at[r], up_r.at[r], sector=lax.rem(s + 1, sectors))

    def downward(r):
        return send(whole.at[0, slab(r)], down_in.at[slab(r)], down_s.at[r], down_r.at[r],
                    sector=lax.rem(s + sectors - 1, sectors))

    def scatter(r, source):
        return send(acc.at[slab(r)], rs_in.at[source], rs_s.at[r], rs_r.at[source], term=r)

    @pl.loop(0, terms)
    def _(k):
        r = lax.rem(t + 1 + k, terms)

        @pl.when(s + 1 < sectors)
        def _():
            upward(r).start()

        @pl.when(s > 0)
        def _():
            downward(r).start()

    @pl.loop(0, terms)
    def _(k):
        r = lax.rem(t + 1 + k, terms)
        acc[slab(r)] = whole[1, slab(r)]

        @pl.when(s > 0)
        def _():
            upward(r).wait_recv()
            acc[slab(r)] += up_in[slab(r)]

        @pl.when(s + 1 < sectors)
        def _():
            downward(r).wait_recv()
            acc[slab(r)] += down_in[slab(r)]

        @pl.when(k < terms - 1)
        def _():
            scatter(r, t).start()

    image[...] = acc[slab(t)]

    @pl.loop(0, terms - 1)
    def _(k):
        j = lax.rem(t + terms - 1 - k, terms)
        scatter(j, j).wait_recv()
        image[...] += rs_in[j]

    def finish():
        @pl.loop(0, terms)
        def _(k):
            r = lax.rem(t + 1 + k, terms)

            @pl.when(s + 1 < sectors)
            def _():
                upward(r).wait_send()

            @pl.when(s > 0)
            def _():
                downward(r).wait_send()

            @pl.when(k < terms - 1)
            def _():
                scatter(r, t).wait_send()

    return finish


def exchange_scratch(width, terms):
    rows = width // terms
    return [pltpu.VMEM((width, width), F32)] * 3 + [pltpu.VMEM((terms, rows, width), F32)] + [
        pltpu.SemaphoreType.DMA((terms,))
    ] * 6


def first_kernel(whole, wave, precond, image, correction, full, *scratch):
    bufs, (gather, own, mid, term_in, sector_in, ag_s, ag_r, ts_s, ts_r, ss_s, ss_r) = scratch[:10], scratch[10:]
    terms, sectors = lax.axis_size("term"), lax.axis_size("sector")
    t, s = lax.axis_index("term"), lax.axis_index("sector")
    rows = image.shape[0]
    greet()
    finish = exchange(whole, image, bufs)

    w = wave[pl.ds(pl.multiple_of(t * rows, rows), rows)]
    f = image[...]
    p = precond[...]
    wf, ww = w * f, w * w

    def lanes(x):
        line = jnp.sum(x, axis=0, keepdims=True)
        return sum(line[:, c : c + 128] for c in range(0, line.shape[1], 128))

    own[...] = jnp.zeros_like(own)
    for i, x in enumerate((wf, ww, wf * p, ww * p)):
        own[i : i + 1] = lanes(x)

    def to_term(k):
        return send(own, term_in.at[k - 1], ts_s.at[k - 1], ts_r.at[k - 1], term=lax.rem(t + k, terms))

    def to_sector(k):
        return send(mid, sector_in.at[k - 1], ss_s.at[k - 1], ss_r.at[k - 1], sector=lax.rem(s + k, sectors))

    for k in range(1, terms):
        to_term(k).start()
    total = own[...]
    for k in range(1, terms):
        to_term(k).wait_recv()
        total += term_in[k - 1]
    mid[...] = total
    for k in range(1, sectors):
        to_sector(k).start()
    for k in range(1, sectors):
        to_sector(k).wait_recv()
        total += sector_in[k - 1]
    cross, norm, a, b = (jnp.sum(total[i : i + 1], axis=1, keepdims=True) for i in range(4))
    rayleigh = cross / norm
    share = (a - rayleigh * b) / norm
    gather[t] = p * (f - rayleigh * w) - share * w

    def spread(r, source):
        return send(gather.at[source], gather.at[source], ag_s.at[r], ag_r.at[source], term=r)

    for k in range(1, terms):
        spread(lax.rem(t + k, terms), t).start()
    correction[...] = gather[t]
    full[pl.ds(pl.multiple_of(t * rows, rows), rows)] = gather[t]
    for k in range(1, terms):
        j = lax.rem(t + terms - k, terms)
        spread(j, j).wait_recv()
        full[pl.ds(pl.multiple_of(j * rows, rows), rows)] = gather[j]
    finish()
    for k in range(1, terms):
        spread(lax.rem(t + k, terms), t).wait_send()
        to_term(k).wait_send()
    for k in range(1, sectors):
        to_sector(k).wait_send()


def second_kernel(whole, image, *scratch):
    greet()
    exchange(whole, image, scratch)()


def per_device(wavefunction, precond, left_ops, right_ops, out_sector, live_counts):
    terms, sectors = lax.axis_size("term"), lax.axis_size("sector")
    width = wavefunction.shape[1]
    rows = width // terms
    center = wavefunction[0]
    slab = jax.ShapeDtypeStruct((rows, width), F32)
    whole = all_terms(center, left_ops, right_ops, out_sector, live_counts)
    tile = pltpu.VMEM((8, 128), F32)
    dma = pltpu.SemaphoreType.DMA
    first_image, correction, full = pl.pallas_call(
        first_kernel,
        out_shape=(slab, slab, jax.ShapeDtypeStruct((width, width), F32)),
        in_specs=[VMEM] * 3,
        out_specs=(VMEM,) * 3,
        scratch_shapes=exchange_scratch(width, terms) + [
            pltpu.VMEM((terms, rows, width), F32), tile, tile,
            pltpu.VMEM((terms - 1, 8, 128), F32), pltpu.VMEM((sectors - 1, 8, 128), F32),
            dma((terms,)), dma((terms,)), dma((terms - 1,)), dma((terms - 1,)),
            dma((sectors - 1,)), dma((sectors - 1,)),
        ],
        compiler_params=pltpu.CompilerParams(collective_id=0, has_side_effects=True, vmem_limit_bytes=32 << 20),
    )(whole, center, precond[0])
    whole = all_terms(full, left_ops, right_ops, out_sector, live_counts)
    second_image = pl.pallas_call(
        second_kernel,
        out_shape=slab,
        in_specs=[VMEM],
        out_specs=VMEM,
        scratch_shapes=exchange_scratch(width, terms),
        compiler_params=pltpu.CompilerParams(collective_id=1, has_side_effects=True, vmem_limit_bytes=32 << 20),
    )(whole)
    return (first_image[None], correction[None], second_image[None])


def solution(mesh):
    placed = (
        P("sector", None, None),
        P("sector", "term", None),
        P("sector", "term", None, None),
        P("sector", "term", None, None),
        P("sector", "term"),
        P("sector", "term"),
    )
    return jax.shard_map(
        per_device,
        mesh=mesh,
        in_specs=placed,
        out_specs=(P("sector", "term", None), P("sector", "term", None), P("sector", "term", None)),
        check_vma=False,
    )
```

```python
import functools

import jax
import jax.numpy as jnp
from jax import lax
from jax.experimental import pallas as pl
from jax.experimental.pallas import tpu as pltpu
from jax.sharding import PartitionSpec as P

F32 = jnp.float32
MESH = pl.DeviceIdType.MESH
VMEM = pl.BlockSpec(memory_space=pltpu.VMEM)


def split(x):
    high = x.astype(jnp.bfloat16)
    return high, (x - high.astype(F32)).astype(jnp.bfloat16)


def product(a_high, a_low, b_high, b_low):
    dot = functools.partial(jnp.dot, preferred_element_type=F32)
    return dot(a_high, b_high) + dot(a_high, b_low) + dot(a_low, b_high)


def terms_kernel(target, count, v_ref, left_ref, right_ref, out_ref, v_high, v_low, r_high, r_low):
    slot = pl.program_id(0)
    width = v_ref.shape[0]
    piece = min(256, width)

    @pl.when(slot == 0)
    def _():
        out_ref[...] = jnp.zeros_like(out_ref)
        v_high[...], v_low[...] = split(v_ref[...])

    @pl.when(slot < count[0, 0])
    def _():
        place = target[0, slot] - lax.axis_index("sector") + 1
        r_high[...], r_low[...] = split(right_ref[...])
        for start in range(0, width, piece):
            rows = pl.ds(start, piece)
            left_high, left_low = split(left_ref[rows])
            inner = product(left_high, left_low, v_high[...], v_low[...])
            in_high, in_low = split(inner)
            out_ref[place, rows] += product(in_high, in_low, r_high[...], r_low[...])


def all_terms(vector, left_ops, right_ops, out_sector, live_counts):
    slots, width = left_ops.shape[1], left_ops.shape[2]

    def live(j, target, count):
        return (0, jnp.minimum(j, count[0, 0] - 1), 0, 0)

    return pl.pallas_call(
        terms_kernel,
        out_shape=jax.ShapeDtypeStruct((3, width, width), F32),
        grid_spec=pltpu.PrefetchScalarGridSpec(
            num_scalar_prefetch=2,
            grid=(slots,),
            in_specs=[
                pl.BlockSpec((width, width), lambda j, a, b: (0, 0)),
                pl.BlockSpec((None, None, width, width), live),
                pl.BlockSpec((None, None, width, width), live),
            ],
            out_specs=pl.BlockSpec((3, width, width), lambda j, a, b: (0, 0, 0)),
            scratch_shapes=[pltpu.VMEM((width, width), jnp.bfloat16)] * 4,
        ),
        compiler_params=pltpu.CompilerParams(dimension_semantics=("arbitrary",), vmem_limit_bytes=58 << 20),
    )(out_sector, live_counts, vector, left_ops, right_ops)


def send(source, target, send_sem, recv_sem, **where):
    return pltpu.make_async_remote_copy(
        src_ref=source, dst_ref=target, send_sem=send_sem, recv_sem=recv_sem,
        device_id=where, device_id_type=MESH,
    )


def greet():
    terms, sectors = lax.axis_size("term"), lax.axis_size("sector")
    t, s = lax.axis_index("term"), lax.axis_index("sector")
    barrier = pltpu.get_barrier_semaphore()
    for k in range(1, terms):
        pl.semaphore_signal(barrier, inc=1, device_id={"term": lax.rem(t + k, terms)}, device_id_type=MESH)
    for k in range(1, sectors):
        pl.semaphore_signal(barrier, inc=1, device_id={"sector": lax.rem(s + k, sectors)}, device_id_type=MESH)
    pl.semaphore_wait(barrier, terms + sectors - 2)


def exchange(whole, image, bufs):
    up_in, down_in, acc, rs_in, up_s, up_r, down_s, down_r, rs_s, rs_r = bufs
    terms, sectors = lax.axis_size("term"), lax.axis_size("sector")
    t, s = lax.axis_index("term"), lax.axis_index("sector")
    rows = whole.shape[1] // terms

    def slab(r):
        return pl.ds(pl.multiple_of(r * rows, rows), rows)

    def upward(r):
        return send(whole.at[2, slab(r)], up_in.at[slab(r)], up_s.at[r], up_r.at[r], sector=lax.rem(s + 1, sectors))

    def downward(r):
        return send(whole.at[0, slab(r)], down_in.at[slab(r)], down_s.at[r], down_r.at[r],
                    sector=lax.rem(s + sectors - 1, sectors))

    def scatter(r, source):
        return send(acc.at[slab(r)], rs_in.at[source], rs_s.at[r], rs_r.at[source], term=r)

    @pl.loop(0, terms)
    def _(k):
        r = lax.rem(t + 1 + k, terms)

        @pl.when(s + 1 < sectors)
        def _():
            upward(r).start()

        @pl.when(s > 0)
        def _():
            downward(r).start()

    @pl.loop(0, terms)
    def _(k):
        r = lax.rem(t + 1 + k, terms)
        acc[slab(r)] = whole[1, slab(r)]

        @pl.when(s > 0)
        def _():
            upward(r).wait_recv()
            acc[slab(r)] += up_in[slab(r)]

        @pl.when(s + 1 < sectors)
        def _():
            downward(r).wait_recv()
            acc[slab(r)] += down_in[slab(r)]

        @pl.when(k < terms - 1)
        def _():
            scatter(r, t).start()

    image[...] = acc[slab(t)]

    @pl.loop(0, terms - 1)
    def _(k):
        j = lax.rem(t + terms - 1 - k, terms)
        scatter(j, j).wait_recv()
        image[...] += rs_in[j]

    def finish():
        @pl.loop(0, terms)
        def _(k):
            r = lax.rem(t + 1 + k, terms)

            @pl.when(s + 1 < sectors)
            def _():
                upward(r).wait_send()

            @pl.when(s > 0)
            def _():
                downward(r).wait_send()

            @pl.when(k < terms - 1)
            def _():
                scatter(r, t).wait_send()

    return finish


def exchange_scratch(width, terms):
    rows = width // terms
    return [pltpu.VMEM((width, width), F32)] * 3 + [pltpu.VMEM((terms, rows, width), F32)] + [
        pltpu.SemaphoreType.DMA((terms,))
    ] * 6


def first_kernel(whole, wave, precond, image, correction, full, *scratch):
    bufs, (gather, own, mid, term_in, sector_in, ag_s, ag_r, ts_s, ts_r, ss_s, ss_r) = scratch[:10], scratch[10:]
    terms, sectors = lax.axis_size("term"), lax.axis_size("sector")
    t, s = lax.axis_index("term"), lax.axis_index("sector")
    rows = image.shape[0]
    greet()
    finish = exchange(whole, image, bufs)

    w = wave[pl.ds(pl.multiple_of(t * rows, rows), rows)]
    f = image[...]
    p = precond[...]
    wf, ww = w * f, w * w

    def lanes(x):
        line = jnp.sum(x, axis=0, keepdims=True)
        return sum(line[:, c : c + 128] for c in range(0, line.shape[1], 128))

    own[...] = jnp.zeros_like(own)
    for i, x in enumerate((wf, ww, wf * p, ww * p)):
        own[i : i + 1] = lanes(x)

    def to_term(k):
        return send(own, term_in.at[k - 1], ts_s.at[k - 1], ts_r.at[k - 1], term=lax.rem(t + k, terms))

    def to_sector(k):
        return send(mid, sector_in.at[k - 1], ss_s.at[k - 1], ss_r.at[k - 1], sector=lax.rem(s + k, sectors))

    for k in range(1, terms):
        to_term(k).start()
    total = own[...]
    for k in range(1, terms):
        to_term(k).wait_recv()
        total += term_in[k - 1]
    mid[...] = total
    for k in range(1, sectors):
        to_sector(k).start()
    for k in range(1, sectors):
        to_sector(k).wait_recv()
        total += sector_in[k - 1]
    cross, norm, a, b = (jnp.sum(total[i : i + 1], axis=1, keepdims=True) for i in range(4))
    rayleigh = cross / norm
    share = (a - rayleigh * b) / norm
    gather[t] = p * (f - rayleigh * w) - share * w

    def spread(r, source):
        return send(gather.at[source], gather.at[source], ag_s.at[r], ag_r.at[source], term=r)

    for k in range(1, terms):
        spread(lax.rem(t + k, terms), t).start()
    correction[...] = gather[t]
    full[pl.ds(pl.multiple_of(t * rows, rows), rows)] = gather[t]
    for k in range(1, terms):
        j = lax.rem(t + terms - k, terms)
        spread(j, j).wait_recv()
        full[pl.ds(pl.multiple_of(j * rows, rows), rows)] = gather[j]
    finish()
    for k in range(1, terms):
        spread(lax.rem(t + k, terms), t).wait_send()
        to_term(k).wait_send()
    for k in range(1, sectors):
        to_sector(k).wait_send()


def second_kernel(whole, image, *scratch):
    greet()
    exchange(whole, image, scratch)()


def per_device(wavefunction, precond, left_ops, right_ops, out_sector, live_counts):
    terms, sectors = lax.axis_size("term"), lax.axis_size("sector")
    width = wavefunction.shape[1]
    rows = width // terms
    center = wavefunction[0]
    slab = jax.ShapeDtypeStruct((rows, width), F32)
    whole = all_terms(center, left_ops, right_ops, out_sector, live_counts)
    tile = pltpu.VMEM((8, 128), F32)
    dma = pltpu.SemaphoreType.DMA
    first_image, correction, full = pl.pallas_call(
        first_kernel,
        out_shape=(slab, slab, jax.ShapeDtypeStruct((width, width), F32)),
        in_specs=[VMEM] * 3,
        out_specs=(VMEM,) * 3,
        scratch_shapes=exchange_scratch(width, terms) + [
            pltpu.VMEM((terms, rows, width), F32), tile, tile,
            pltpu.VMEM((terms - 1, 8, 128), F32), pltpu.VMEM((sectors - 1, 8, 128), F32),
            dma((terms,)), dma((terms,)), dma((terms - 1,)), dma((terms - 1,)),
            dma((sectors - 1,)), dma((sectors - 1,)),
        ],
        compiler_params=pltpu.CompilerParams(collective_id=0, has_side_effects=True, vmem_limit_bytes=32 << 20),
    )(whole, center, precond[0])
    whole = all_terms(full, left_ops, right_ops, out_sector, live_counts)
    second_image = pl.pallas_call(
        second_kernel,
        out_shape=slab,
        in_specs=[VMEM],
        out_specs=VMEM,
        scratch_shapes=exchange_scratch(width, terms),
        compiler_params=pltpu.CompilerParams(collective_id=1, has_side_effects=True, vmem_limit_bytes=32 << 20),
    )(whole)
    return (first_image[None], correction[None], second_image[None])


def solution(mesh):
    placed = (
        P("sector", None, None),
        P("sector", "term", None),
        P("sector", "term", None, None),
        P("sector", "term", None, None),
        P("sector", "term"),
        P("sector", "term"),
    )
    return jax.shard_map(
        per_device,
        mesh=mesh,
        in_specs=placed,
        out_specs=(P("sector", "term", None), P("sector", "term", None), P("sector", "term", None)),
        check_vma=False,
    )
```
